32 devices in a mesh: zero: 4 (over z), width: 4 (over y, x), unit: 2 (over core).
Axes of the slice: x: 2, y: 2, z: 4, core: 2. Of those that a mesh axis runs over, the one named last changes fastest.
Arguments:
- grad_stack: float32 [64, 128, 2048], P('unit', 'zero', 'width'), parts along dimension 0, may hold values from -6 to 6
- moment_stack: float32 [64, 128, 2048], P('unit', 'zero', 'width'), parts along dimension 0, may hold values from -6 to 6
- weight_stack: float32 [64, 128, 2048], P('unit', 'zero', 'width'), parts along dimension 0, may hold values from -0.1875 to 0.1875
Outputs:
- new_weights: float32 [64, 128, 2048], P('unit', 'zero', 'width'), parts along dimension 0
- new_momentum: float32 [64, 128, 2048], P('unit', 'zero', 'width'), parts along dimension 0
The draws below stay inside these ranges and needn't reach their ends.
There are 2 independent parts, one for each index of `unit`. The reference program is written for one: setup_inputs(seed, part) draws one part's arguments, and reference() takes and returns one part's arrays. A program takes and returns all parts, laid end to end along the dimension named above; each array names one. Nothing has to cross between parts.
All inputs are finite; a program needn't handle non-finite values.
Results may differ from the reference program's by a relative error of at most 0.0001.
Values sent between devices are 32-bit elements; how exact they have to be, the bound alone decides.
No kernel may reach another device: no remote copies, remote signals or barrier semaphores. Data moves between devices by JAX's collectives and lax.ppermute only.
A program may use at most 64 MiB of HBM per device.

```python
import jax
import jax.numpy as jnp
from jax import lax

SIDE = 128
WIDE = 2048
MATS = 32
ITERS = 3


def shard_levels(key, dims, shards, least, top_value):
    def one(dim, parts):
        steps = jax.random.uniform(jax.random.fold_in(jax.random.fold_in(key, 6), dim), (parts,), jnp.float32, least / len(shards), top_value / len(shards))
        return jnp.repeat(jnp.exp(steps), dims[dim] // parts).reshape((-1,) + (1,) * (len(dims) - dim - 1))

    loudness = one(*shards[0])
    for cut in shards[1:]:
        loudness = loudness * one(*cut)
    return loudness


def noise(key, shape, width, most, cuts=(), held_as=jnp.bfloat16):
    entries = width * jax.random.normal(key, shape, jnp.float32)
    if cuts:
        entries = entries * shard_levels(key, shape, cuts, -0.22, 0.18)
    return jnp.clip(entries, -most, most).astype(held_as)


def setup_inputs(seed: int = 0, part: int = 0) -> dict:
    splits = jax.random.split(jax.random.key(seed), 4)
    own_keys = jax.random.split(jax.random.fold_in(splits[3], part), 4)
    return {
        "grad_stack": noise(own_keys[0], (MATS, SIDE, WIDE), 1.0, 6.0, ((1, 4), (2, 4)), jnp.float32),
        "moment_stack": noise(own_keys[1], (MATS, SIDE, WIDE), 1.0, 6.0, ((1, 4), (2, 4)), jnp.float32),
        "weight_stack": noise(own_keys[2], (MATS, SIDE, WIDE), 0.03, 0.1875, ((1, 4), (2, 4)), jnp.float32),
    }


hold_rate = 0.95
learn_rate = 0.8
decay_rate = 0.1

def reference(grad_stack, moment_stack, weight_stack):
    new_momentum = hold_rate * moment_stack + grad_stack

    def orthogonal_one(stack):
        iterate = stack[None]
        iterate = iterate * lax.rsqrt(lax.optimization_barrier(jnp.sum(iterate * iterate, axis=(1, 2), keepdims=True)) + 1e-06)
        for step in range(ITERS):
            gram = jnp.einsum('mik,mjk->mij', iterate, iterate, precision=lax.Precision.HIGHEST)
            mixed = -4.775 * gram + 2.0315 * jnp.einsum('mij,mjk->mik', gram, gram, precision=lax.Precision.HIGHEST)
            iterate = 3.4445 * iterate + jnp.einsum('mij,mjk->mik', mixed, iterate, precision=lax.Precision.HIGHEST)
        return iterate[0]
    iterate = lax.map(orthogonal_one, new_momentum)
    new_weights = (1.0 - learn_rate * decay_rate) * weight_stack - learn_rate * iterate
    return (new_weights, new_momentum)
```

```python
import jax
import jax.numpy as jnp
from jax import lax
from jax.experimental import pallas as pl
from jax.experimental.pallas import tpu as pltpu
from jax.sharding import PartitionSpec as P

ITERS = 3
CHUNKS = 2
DIRECT = 4

hold_rate = 0.95
learn_rate = 0.8
decay_rate = 0.1


def mm(a, b, dims=((1,), (0,))):
    return lax.dot_general(
        a, b, (dims, ((), ())),
        precision=lax.Precision.HIGHEST,
        preferred_element_type=jnp.float32,
    )


def gram_kernel(*refs):
    *pieces, out = refs
    for i in range(out.shape[0]):
        x = jnp.concatenate([p[i] for p in pieces], axis=0)
        out[i] = mm(x, x, ((1,), (1,)))


def gram(pieces):
    m = pieces[0].shape[0]
    side = sum(p.shape[1] for p in pieces)
    return pl.pallas_call(
        gram_kernel,
        out_shape=jax.ShapeDtypeStruct((m, side, side), jnp.float32),
        name="gram",
    )(*pieces)


def apply_kernel(parts, count, *refs):
    partial, pieces, outs = refs[:parts], refs[parts : parts + count], refs[parts + count :]
    m, side, _ = partial[0].shape
    eye = (
        lax.broadcasted_iota(jnp.int32, (side, side), 0)
        == lax.broadcasted_iota(jnp.int32, (side, side), 1)
    ).astype(jnp.float32)
    each = range(m)
    grams, scales = [], []
    for i in each:
        g = partial[0][i]
        for p in partial[1:]:
            g = g + p[i]
        total = jnp.sum(g * eye, axis=(0, 1), keepdims=True)
        s = lax.rsqrt(total + 1e-06)
        scales.append(s)
        grams.append(g * (s * s))
    product = None
    for step in range(ITERS):
        squares = [mm(grams[i], grams[i]) for i in each]
        mixed = [3.4445 * eye + (-4.775 * grams[i] + 2.0315 * squares[i]) for i in each]
        product = mixed if product is None else [mm(mixed[i], product[i]) for i in each]
        if step + 1 < ITERS:
            halves = [mm(mixed[i], grams[i]) for i in each]
            grams = [mm(halves[i], mixed[i]) for i in each]
    for i in each:
        x = jnp.concatenate([p[i] for p in pieces], axis=0)
        y = mm(product[i] * scales[i], x)
        at = 0
        for o in outs:
            o[i] = y[at : at + o.shape[1]]
            at += o.shape[1]


def apply(partial, pieces):
    return pl.pallas_call(
        lambda *refs: apply_kernel(len(partial), len(pieces), *refs),
        out_shape=[jax.ShapeDtypeStruct(p.shape, jnp.float32) for p in pieces],
        name="apply",
    )(*partial, *pieces)


def swap(v, axis, n, k):
    return lax.ppermute(v, axis, [(i, i ^ k) for i in range(n)])


def total_over(v, axis, n):
    if n & (n - 1):
        return [lax.psum(v, axis)]
    return [v] + [swap(v, axis, n, k) for k in range(1, n)]


def body(nz, nw, grad_stack, moment_stack, weight_stack):
    mats, rows, cols = grad_stack.shape
    own = mats // nz
    chunks = CHUNKS if own % CHUNKS == 0 else 1
    m = own // chunks
    z = lax.axis_index("zero")
    direct = nz <= DIRECT and nz & (nz - 1) == 0
    new_momentum = hold_rate * moment_stack + grad_stack
    keep = 1.0 - learn_rate * decay_rate

    def part(v, k, c):
        return lax.dynamic_slice_in_dim(v, (z ^ k) * own + c * m, m, axis=0)

    order = sorted(range(1, nz), reverse=True)
    gathered = []
    for c in range(chunks):
        if direct:
            sent = {
                k: hold_rate * part(moment_stack, k, c) + part(grad_stack, k, c)
                for k in range(nz)
            }
            got = {k: swap(sent[k], "zero", nz, k) for k in order}
            gathered.append([sent[0]] + [got[k] for k in range(1, nz)])
        else:
            v = new_momentum.reshape(nz, own, rows, cols)[:, c * m : (c + 1) * m]
            v = lax.all_to_all(v, "zero", split_axis=0, concat_axis=0, tiled=True)
            gathered.append([jnp.swapaxes(v, 0, 1).reshape(m, nz * rows, cols)])
    back = []
    for c in range(chunks):
        partial = total_over(gram(gathered[c]), "width", nw)
        done = apply(partial, gathered[c])
        if direct:
            got = {k: swap(done[k], "zero", nz, k) for k in order}
            got[0] = done[0]
            back.append(got)
        else:
            v = jnp.swapaxes(done[0].reshape(m, nz, rows, cols), 0, 1)
            back.append(lax.all_to_all(v, "zero", split_axis=0, concat_axis=0, tiled=True))
    if direct:
        new_weights = jnp.zeros_like(weight_stack)
        for c in range(chunks):
            for k in [0] + order:
                new = keep * part(weight_stack, k, c) - learn_rate * back[c][k]
                new_weights = lax.dynamic_update_slice_in_dim(
                    new_weights, new, (z ^ k) * own + c * m, axis=0
                )
    else:
        whole = jnp.concatenate(back, axis=1).reshape(mats, rows, cols)
        new_weights = keep * weight_stack - learn_rate * whole
    return (new_weights, new_momentum)


def solution(mesh):
    nz, nw = mesh.shape["zero"], mesh.shape["width"]
    return jax.shard_map(
        lambda *args: body(nz, nw, *args),
        mesh=mesh,
        in_specs=(
            P("unit", "zero", "width"),
            P("unit", "zero", "width"),
            P("unit", "zero", "width"),
        ),
        out_specs=(P("unit", "zero", "width"), P("unit", "zero", "width")),
        check_vma=False,
    )
```
